512 devices in a mesh: section: 8 (over y_lo, core), dp: 64 (over y_hi, x, z).
Axes of the slice: x: 4, y: 8 (y_hi: 2, y_lo: 4; y = y_hi * 4 + y_lo), z: 8, core: 2. Of those that a mesh axis runs over, the one named last changes fastest.
Arguments:
- tokens: int32 [8, 5120], P(None, 'dp'), may hold values from 0 to 255
- doc_patches: int32 [8], replicated, may hold values from 160 to 640, as said below
- global_embed: bfloat16 [8, 640, 4096], P('section', 'dp'), may hold values from -6 to 6
- byte_table: bfloat16 [256, 1024], replicated, may hold values from -6 to 6
- w_qkv: bfloat16 [8, 1024, 3072], P('section', 'dp'), may hold values from -0.1875 to 0.1875
- w_out: bfloat16 [8, 1024, 1024], P('section', 'dp'), may hold values from -0.1875 to 0.1875
- layer_gain: bfloat16 [8, 1024], P('section'), may hold values from 0.099609375 to 1.8984375
- w_global: bfloat16 [512, 1024], P(None, 'dp'), may hold values from -0.25 to 0.25
- final_gain: bfloat16 [1024], replicated, may hold values from 0.099609375 to 1.8984375
- w_head: bfloat16 [256, 1024], P(None, 'dp'), may hold values from -0.59765625 to 0.59765625
Outputs:
- logits: bfloat16 [8, 5120, 256], P('section', 'dp')
The draws below stay inside these ranges and needn't reach their ends.
Inputs may be any that keep to these rules, and one draw needn't show every extreme that they name: Patches from index doc_patches[m] on are padding of micro-batch m; the micro-batches' counts differ from one another.
All inputs are finite; a program needn't handle non-finite values.
Results may differ from the reference program's by a relative error of at most 0.014.
Values may be sent and summed in bfloat16 or wider, within the bound.
No kernel may reach another device: no remote copies, remote signals or barrier semaphores. Data moves between devices by JAX's collectives and lax.ppermute only.
A program may use at most 64 MiB of HBM per device.

```python
import jax
import jax.numpy as jnp
from jax import lax

D = 1024
HEADS = 16
VOCAB = 256
GLOBAL_WIDTH = 4096
PATCH = 8
GLOBAL_POS = 512
PATCHES = 640
MICRO = 8
N_SECTION = 8


def draw_doc_patches(key, part):
    lowest = PATCHES // 4
    span = PATCHES - lowest + 1
    order = jax.random.permutation(jax.random.fold_in(key, 17), span)
    return (order[:MICRO] + lowest).astype(jnp.int32)


def set_ends(drawn, rng, least, largest):
    spot = [jax.random.randint(jax.random.fold_in(rng, axis), (), 0, length) for axis, length in enumerate(drawn.shape)]
    longest = drawn.shape.index(max(drawn.shape))
    neighbour = spot[:longest] + [(spot[longest] + 1) % drawn.shape[longest]] + spot[longest + 1:]
    return drawn.at[tuple(spot)].set(least).at[tuple(neighbour)].set(largest)


def shard_levels(rng, shape, cuts, least, high):
    loudness, own = 1.0, jax.random.fold_in(rng, 6)
    for position, parts in cuts:
        draws = jnp.exp(jax.random.uniform(jax.random.fold_in(own, position), (parts,), jnp.float32, least / len(cuts), high / len(cuts)))
        loudness = loudness * jnp.repeat(draws, shape[position] // parts).reshape([-1 if axis == position else 1 for axis in range(len(shape))])
    return loudness


def scatter_about(stream_key, extent, deviation, limit, pieces=(), kind=jnp.bfloat16):
    drawn = jax.random.normal(stream_key, extent, jnp.float32) * deviation
    if len(pieces) > 0:
        drawn = shard_levels(stream_key, extent, pieces, -0.22, 0.18) * drawn
    return jnp.clip(drawn, min=-limit, max=limit).astype(kind)


def setup_inputs(seed: int = 0) -> dict:
    seeds = jax.random.split(jax.random.key(seed), 11)
    tokens = set_ends(jax.random.randint(seeds[0], (MICRO, PATCHES * PATCH), 0, VOCAB), jax.random.fold_in(seeds[0], 1), 0, VOCAB - 1).astype(jnp.int32)
    doc_patches = draw_doc_patches(jax.random.fold_in(seeds[10], 71), 0)
    global_embed = scatter_about(seeds[2], (MICRO, PATCHES, GLOBAL_WIDTH), 1.0, 6.0, ((0, 8), (1, 64)))
    byte_table = scatter_about(seeds[3], (VOCAB, D), 1.0, 6.0)
    w_qkv = scatter_about(seeds[4], (N_SECTION, D, 3 * D), D ** -0.5, 0.1875, ((0, 8), (1, 64)))
    w_out = scatter_about(seeds[5], (N_SECTION, D, D), D ** -0.5, 0.1875, ((0, 8), (1, 64)))
    layer_gain = jnp.clip(1.0 + 0.18 * jax.random.normal(seeds[6], (N_SECTION, D), jnp.float32), 0.099609375, 1.8984375).astype(jnp.bfloat16)
    w_global = scatter_about(seeds[7], (GLOBAL_POS, D), GLOBAL_POS ** -0.5, 0.25, ((1, 64),))
    final_gain = jnp.clip(1.0 + 0.18 * jax.random.normal(seeds[8], (D,), jnp.float32), 0.099609375, 1.8984375).astype(jnp.bfloat16)
    w_head = scatter_about(seeds[9], (VOCAB, D), 0.1, 0.59765625, ((1, 64),))
    return {"tokens": tokens, "doc_patches": doc_patches, "global_embed": global_embed, "byte_table": byte_table, "w_qkv": w_qkv, "w_out": w_out, "layer_gain": layer_gain, "w_global": w_global, "final_gain": final_gain, "w_head": w_head}


def norm_rows(hidden, norm_gain):
    scale = lax.rsqrt(lax.optimization_barrier(jnp.mean(hidden * hidden, axis=-1, keepdims=True)) + 1e-06)
    return (hidden * scale * norm_gain.astype(jnp.float32)).astype(jnp.bfloat16)

def attend_layer(inputs, global_add, norm_gain, qkv_weight, out_weight):
    hidden = inputs.astype(jnp.float32) + global_add.astype(jnp.float32)
    normed = norm_rows(hidden, norm_gain)
    projected = jnp.dot(normed, qkv_weight, preferred_element_type=jnp.float32).astype(jnp.bfloat16)
    model_width = inputs.shape[1]
    head_dim = model_width // HEADS
    patch_count = inputs.shape[0] // PATCH

    def split_heads(block):
        return block.reshape(patch_count, PATCH, HEADS, head_dim).astype(jnp.float32)
    queries = split_heads(projected[:, :model_width])
    key_rows = split_heads(projected[:, model_width:2 * model_width])
    value_rows = split_heads(projected[:, 2 * model_width:])
    scores = jnp.einsum('pqhd,pkhd->phqk', queries, key_rows) * head_dim ** (-0.5)
    causal = jnp.tril(jnp.ones((PATCH, PATCH), dtype=jnp.bool_))
    scores = jnp.where(causal, scores, -1e+30)
    weights = jax.nn.softmax(scores, axis=-1).astype(jnp.bfloat16)
    context = jnp.einsum('phqk,pkhd->pqhd', weights.astype(jnp.float32), value_rows)
    context = context.astype(jnp.bfloat16).reshape(inputs.shape[0], model_width)
    return (hidden + jnp.dot(context, out_weight, preferred_element_type=jnp.float32)).astype(jnp.bfloat16)

def previous_bytes(byte_ids):
    blocks = byte_ids.reshape(-1, PATCH)
    shifted = jnp.concatenate([jnp.zeros((blocks.shape[0], 1), jnp.int32), blocks[:, :-1]], axis=1)
    return shifted.reshape(-1)

def reference(tokens, doc_patches, global_embed, byte_table, w_qkv, w_out, layer_gain, w_global, final_gain, w_head):
    row_total = PATCHES * PATCH
    results = []
    for micro_index in range(MICRO):
        inputs = jnp.take(byte_table, previous_bytes(tokens[micro_index]), axis=0)
        global_rows = global_embed[micro_index].reshape(row_total, GLOBAL_POS)
        global_add = jnp.dot(global_rows, w_global, preferred_element_type=jnp.float32).astype(jnp.bfloat16)
        for section_index in range(N_SECTION):
            inputs = attend_layer(inputs, global_add, layer_gain[section_index], w_qkv[section_index], w_out[section_index])
        final_rows = norm_rows(inputs.astype(jnp.float32), final_gain)
        scores = jnp.dot(final_rows, w_head.T, preferred_element_type=jnp.float32)
        patch_of_row = jnp.arange(row_total, dtype=jnp.int32) // PATCH
        live_rows = patch_of_row < doc_patches[micro_index]
        results.append(jnp.where(live_rows[:, None], scores, 0.0).astype(jnp.bfloat16))
    return jnp.stack(results)
```

```python
import functools

import jax
import jax.numpy as jnp
from jax import lax
from jax.experimental import pallas as pl
from jax.experimental.pallas import tpu as pltpu
from jax.sharding import PartitionSpec as P

HEADS = 16
PATCH = 8
HEAD_DIM = 64
GROUPS = 4


def norm_rows(hidden, gain):
    scale = lax.rsqrt(jnp.mean(hidden * hidden, axis=-1, keepdims=True) + 1e-06)
    return (hidden * scale * gain.astype(jnp.float32)).astype(jnp.bfloat16)


def layer_body(final, t_ref, meta_ref, recv_ref, embed_hbm, add_hbm, gain_ref, final_gain_ref,
               w_hbm, *rest):
    if final:
        out_ref, logits_ref, x_buf, add_buf, ctx_buf, qkv_buf, wo_buf, head_buf, sems, group_sems, out_sems = rest
    else:
        out_ref, x_buf, add_buf, ctx_buf, qkv_buf, wo_buf, sems, group_sems, out_sems = rest
    rows, width = out_ref.shape
    halves, blocks = qkv_buf.shape[1:3]
    lanes = width // GROUPS
    micro_count = add_hbm.shape[0]
    section = meta_ref[0]
    last_section = meta_ref[1]
    micro = t_ref[0] - 2 * section
    active = (micro >= 0) & (micro < micro_count)

    @pl.when(active)
    def _():
        add_copy = pltpu.make_async_copy(add_hbm.at[micro], add_buf, sems.at[0])
        add_copy.start()
        embed_copy = pltpu.make_async_copy(embed_hbm.at[micro], x_buf, sems.at[1])

        @pl.when(section == 0)
        def _():
            embed_copy.start()

        qkv_copies, out_copies = [], []
        per_group = blocks * halves // GROUPS
        for g in range(GROUPS):
            copies = []
            for h in range(halves):
                for p in range(3):
                    copies.append(pltpu.make_async_copy(
                        w_hbm.at[:, h, :, pl.ds(p * width + g * lanes, lanes)],
                        qkv_buf.at[g, h, :, :, pl.ds(p * lanes, lanes)],
                        group_sems.at[g, h * 3 + p]))
            for c in copies:
                c.start()
            qkv_copies.append(copies)
        for h in range(halves):
            copy = pltpu.make_async_copy(
                w_hbm.at[:, h, :, pl.ds(3 * width, width)], wo_buf.at[h], out_sems.at[h])
            copy.start()
            out_copies.append(copy)
        if final:
            head_copies = [pltpu.make_async_copy(
                w_hbm.at[:, h, :, pl.ds(4 * width, 256)], head_buf.at[h], out_sems.at[halves + h])
                for h in range(halves)]

            @pl.when(section == last_section)
            def _():
                for c in head_copies:
                    c.start()

        @pl.when(section == 0)
        def _():
            embed_copy.wait()

        @pl.when(section != 0)
        def _():
            x_buf[...] = recv_ref[...]

        add_copy.wait()
        hidden = x_buf[...].astype(jnp.float32) + add_buf[...].astype(jnp.float32)
        normed = norm_rows(hidden, gain_ref[...])
        row = lax.broadcasted_iota(jnp.int32, (rows, rows), 0)
        col = lax.broadcasted_iota(jnp.int32, (rows, rows), 1)
        seen = (row // PATCH == col // PATCH) & (col <= row)
        in_group = lanes // HEAD_DIM
        seen = jnp.concatenate([seen] * in_group, axis=0)
        head_of = lax.broadcasted_iota(jnp.int32, (rows, lanes), 1) // HEAD_DIM
        for g in range(GROUPS):
            for c in qkv_copies[g]:
                c.wait()
            w = qkv_buf[g].reshape(width, 3 * lanes)
            proj = jnp.dot(normed, w, preferred_element_type=jnp.float32).astype(jnp.bfloat16)
            q, k, v = proj[:, :lanes], proj[:, lanes:2 * lanes], proj[:, 2 * lanes:]
            zero = jnp.zeros_like(q)
            spread = jnp.concatenate([jnp.where(head_of == j, q, zero) for j in range(in_group)], axis=0)
            scores = lax.dot_general(spread, k, (((1,), (1,)), ((), ())),
                                     preferred_element_type=jnp.float32) * HEAD_DIM ** (-0.5)
            scores = jnp.where(seen, scores, -1e30)
            e = jnp.exp(scores - jnp.max(scores, axis=-1, keepdims=True))
            attn = (e / jnp.sum(e, axis=-1, keepdims=True)).astype(jnp.bfloat16)
            wide = jnp.dot(attn, v, preferred_element_type=jnp.float32)
            ctx = wide[:rows]
            for j in range(1, in_group):
                ctx = jnp.where(head_of == j, wide[j * rows:(j + 1) * rows], ctx)
            ctx_buf[:, g * lanes:(g + 1) * lanes] = ctx.astype(jnp.bfloat16)
        for c in out_copies:
            c.wait()
        mixed = jnp.dot(ctx_buf[...], wo_buf[...].reshape(width, width), preferred_element_type=jnp.float32)
        result = (hidden + mixed).astype(jnp.bfloat16)
        out_ref[...] = result
        if final:
            @pl.when(section == last_section)
            def _():
                for c in head_copies:
                    c.wait()
                final_rows = norm_rows(out_ref[...].astype(jnp.float32), final_gain_ref[...])
                scores = jnp.dot(final_rows, head_buf[...].reshape(width, -1),
                                 preferred_element_type=jnp.float32)
                patch = meta_ref[2] + lax.broadcasted_iota(jnp.int32, scores.shape, 0) // PATCH
                live = patch < meta_ref[3 + micro]
                logits_ref[...] = jnp.where(live, scores, 0.0).astype(jnp.bfloat16)


def layer_call(t, meta, recv, embeds, adds, gain, final_gain, weights, final):
    rows, width = recv.shape
    blocks, halves = weights.shape[:2]
    vmem = pl.BlockSpec(memory_space=pltpu.VMEM)
    smem = pl.BlockSpec(memory_space=pltpu.SMEM)
    hbm = pl.BlockSpec(memory_space=pl.ANY)
    x_shape = jax.ShapeDtypeStruct((rows, width), jnp.bfloat16)
    scratch = [
        pltpu.VMEM((rows, width), jnp.bfloat16),
        pltpu.VMEM((rows, width), jnp.bfloat16),
        pltpu.VMEM((rows, width), jnp.bfloat16),
        pltpu.VMEM((GROUPS, halves, blocks, 16, 3 * width // GROUPS), jnp.bfloat16),
        pltpu.VMEM((halves, blocks, 16, width), jnp.bfloat16),
    ]
    if final:
        scratch.append(pltpu.VMEM((halves, blocks, 16, 256), jnp.bfloat16))
    scratch += [
        pltpu.SemaphoreType.DMA((2,)),
        pltpu.SemaphoreType.DMA((GROUPS, 3 * halves)),
        pltpu.SemaphoreType.DMA((2 * halves,)),
    ]
    out_shape = [x_shape] + ([jax.ShapeDtypeStruct((rows, 256), jnp.bfloat16)] if final else [])
    return pl.pallas_call(
        functools.partial(layer_body, final),
        out_shape=out_shape,
        in_specs=[smem, smem, vmem, hbm, hbm, vmem, vmem, hbm],
        out_specs=[vmem] * len(out_shape),
        scratch_shapes=scratch,
        compiler_params=pltpu.CompilerParams(vmem_limit_bytes=24 * 2 ** 20),
        cost_estimate=pl.CostEstimate(flops=8 * rows * width * width, bytes_accessed=8 * width * width,
                                      transcendentals=rows * rows * 16),
        name="layer_final" if final else "layer",
    )(t, meta, recv, embeds, adds, gain, final_gain, weights)


def previous_bytes(byte_ids):
    blocks = byte_ids.reshape(-1, PATCH)
    shifted = jnp.concatenate([jnp.zeros((blocks.shape[0], 1), jnp.int32), blocks[:, :-1]], axis=1)
    return shifted.reshape(-1)


def shards(tokens, doc_patches, global_embed, byte_table, w_qkv, w_out, layer_gain, w_global,
           final_gain, w_head):
    sections = lax.axis_size("section")
    columns = lax.axis_size("dp")
    section = lax.axis_index("section")
    column = lax.axis_index("dp")
    micro_count, row_count = tokens.shape
    width = byte_table.shape[1]
    plane = columns // 2

    copies = jnp.broadcast_to(global_embed, (sections, *global_embed.shape[1:]))
    globals_ = lax.all_to_all(copies, "section", split_axis=0, concat_axis=0, tiled=True)

    own = jnp.concatenate([w_qkv[0], w_out[0], w_head.T, w_global.T], axis=1)
    other = lax.ppermute(own, "dp", [(i, (i + plane) % columns) for i in range(columns)])
    low = column < plane
    both = jnp.concatenate([jnp.where(low, own, other), jnp.where(low, other, own)], axis=0)
    teams = [list(range(plane)), list(range(plane, columns))]
    full = lax.all_gather(both, "dp", axis=0, tiled=True, axis_index_groups=teams)
    weights = full.reshape(plane, 2, own.shape[0], own.shape[1])
    glob = jnp.moveaxis(weights[..., 4 * width + w_head.shape[0]:], 1, 0).reshape(width, -1)

    byte_ids = previous_bytes(tokens.reshape(-1))
    one_hot = (byte_ids[:, None] == jnp.arange(byte_table.shape[0], dtype=jnp.int32)[None, :]).astype(jnp.bfloat16)
    embeds = jnp.dot(one_hot, byte_table, preferred_element_type=jnp.float32).astype(jnp.bfloat16)
    embeds = embeds.reshape(micro_count, row_count, width)
    adds = lax.dot_general(globals_.reshape(micro_count * row_count, -1), glob, (((1,), (1,)), ((), ())),
                           preferred_element_type=jnp.float32)
    adds = adds.astype(jnp.bfloat16).reshape(micro_count, row_count, width)

    meta = jnp.concatenate([
        jnp.stack([section, jnp.int32(sections - 1), column * (row_count // PATCH)]).astype(jnp.int32),
        doc_patches])
    final_gain = final_gain.reshape(1, width)
    onward = [(i, i + 1) for i in range(sections - 1)]

    def send(block):
        return lax.ppermute(block, "section", onward)

    def layer(t, recv, final=False):
        t = jnp.full((1,), t, jnp.int32)
        return layer_call(t, meta, recv, embeds, adds, layer_gain, final_gain, weights, final)

    def two_steps(i, state):
        sent, recv = state
        arrived = send(sent)
        (first,) = layer(2 * i, recv)
        again = send(first)
        (second,) = layer(2 * i + 1, arrived)
        return second, again

    blank = jnp.zeros((row_count, width), jnp.bfloat16)
    fill = 2 * (sections - 1)
    sent, recv = lax.fori_loop(0, fill // 2, two_steps, (blank, blank))
    total = None
    for micro in range(micro_count):
        t = fill + micro
        arrived = send(sent) if micro < micro_count - 1 else None
        sent, logits = layer(t, recv, True)
        recv = arrived
        if micro == sections - 1:
            piece = jnp.where(section == micro, logits, jnp.zeros_like(logits))
        else:
            piece = lax.ppermute(logits, "section", [(sections - 1, micro)])
        total = piece if total is None else total + piece
    return total[None]


def solution(mesh):
    in_specs = (
        P(None, "dp"), P(), P("section", "dp", None), P(), P("section", "dp", None),
        P("section", "dp", None), P("section", None), P(None, "dp"), P(), P(None, "dp"),
    )
    return jax.shard_map(shards, mesh=mesh, in_specs=in_specs, out_specs=P("section", "dp", None), check_vma=False)
```

```python
import functools

import jax
import jax.numpy as jnp
from jax import lax
from jax.experimental import pallas as pl
from jax.experimental.pallas import tpu as pltpu
from jax.sharding import PartitionSpec as P

HEADS = 16
PATCH = 8
HEAD_DIM = 64
GROUPS = 4
X_SIZE, Z_SIZE = 4, 8
SHARD = 16
VOCAB = 256
PROJECT_STEPS = 1
ATTEND_STEPS = 1


def norm_rows(hidden, gain):
    scale = lax.rsqrt(jnp.mean(hidden * hidden, axis=-1, keepdims=True) + 1e-06)
    return (hidden * scale * gain.astype(jnp.float32)).astype(jnp.bfloat16)


def pack_body(place_ref, *refs):
    half, x, z = place_ref[0], place_ref[1], place_ref[2]
    near, ups, downs, up_far, down_far = refs[0], refs[1:4], refs[4:7], refs[7], refs[8]
    cross, cross_up, cross_down, cross_far_a, cross_far_b = refs[9:14]
    out_ref, sems = refs[14:]
    copies = []

    def move(source, target):
        copy = pltpu.make_async_copy(source, target, sems.at[len(copies)])
        copy.start()
        copies.append(copy)

    def at_z(step):
        return lax.rem(z + step + Z_SIZE, Z_SIZE)

    def at_x(step):
        return lax.rem(x + step + X_SIZE, X_SIZE)

    move(near, out_ref.at[half, :, z])
    for i in range(3):
        move(ups[i], out_ref.at[half, :, at_z(-1 - i)])
        move(downs[i], out_ref.at[half, :, at_z(1 + i)])
    middle = X_SIZE // 2
    move(up_far, out_ref.at[half, pl.ds(0, middle), at_z(4)])
    move(down_far, out_ref.at[half, pl.ds(middle, middle), at_z(4)])
    middle = Z_SIZE // 2
    move(cross, out_ref.at[1 - half, x])
    move(cross_up, out_ref.at[1 - half, at_x(-1)])
    move(cross_down, out_ref.at[1 - half, at_x(1)])
    move(cross_far_a, out_ref.at[1 - half, at_x(2), pl.ds(0, middle)])
    move(cross_far_b, out_ref.at[1 - half, at_x(2), pl.ds(middle, middle)])
    for copy in copies:
        copy.wait()


def pack_call(place, pieces):
    columns = pieces[0].shape[-1]
    return pl.pallas_call(
        pack_body,
        out_shape=jax.ShapeDtypeStruct((2, X_SIZE, Z_SIZE, SHARD, columns), jnp.bfloat16),
        in_specs=[pl.BlockSpec(memory_space=pltpu.SMEM)] + [pl.BlockSpec(memory_space=pl.ANY)] * len(pieces),
        out_specs=pl.BlockSpec(memory_space=pltpu.VMEM),
        scratch_shapes=[pltpu.SemaphoreType.DMA((len(pieces),))],
        compiler_params=pltpu.CompilerParams(vmem_limit_bytes=16 * 2 ** 20),
        name="pack",
    )(place, *pieces)


def neighbours(axis, step):
    pairs = []
    for h in range(2):
        for x in range(X_SIZE):
            for z in range(Z_SIZE):
                to_h, to_x, to_z = h, x, z
                if axis == "y":
                    to_h = (h + step) % 2
                elif axis == "x":
                    to_x = (x + step) % X_SIZE
                else:
                    to_z = (z + step) % Z_SIZE
                pairs.append(((h * X_SIZE + x) * Z_SIZE + z, (to_h * X_SIZE + to_x) * Z_SIZE + to_z))
    return pairs


def to_team(shard, teams):
    copies = jnp.broadcast_to(shard, (len(teams[0]), *shard.shape))
    return lax.all_to_all(copies, "dp", split_axis=0, concat_axis=0, axis_index_groups=teams, tiled=True)


def gather_plane(own):
    def shift(block, axis, step):
        return lax.ppermute(block, "dp", neighbours(axis, step))

    along_x = [[(h * X_SIZE + x) * Z_SIZE + z for x in range(X_SIZE)] for h in range(2) for z in range(Z_SIZE)]
    along_z = [[r * Z_SIZE + z for z in range(Z_SIZE)] for r in range(2 * X_SIZE)]
    other = shift(own, "y", 1)
    near = to_team(own, along_x)
    ups, downs = [near], [near]
    for _ in range(3):
        ups.append(shift(ups[-1], "z", 1))
        downs.append(shift(downs[-1], "z", -1))
    up_far = shift(ups[-1][:X_SIZE // 2], "z", 1)
    down_far = shift(downs[-1][X_SIZE // 2:], "z", -1)
    cross = to_team(other, along_z)
    cross_up, cross_down = shift(cross, "x", 1), shift(cross, "x", -1)
    far_a = shift(cross_up[:Z_SIZE // 2], "x", 1)
    far_b = shift(cross_down[Z_SIZE // 2:], "x", -1)
    pieces = [near, *ups[1:], *downs[1:], up_far, down_far, cross, cross_up, cross_down, far_a, far_b]
    return pieces, near


def add_body(embed_ref, w_ref, out_ref):
    width = out_ref.shape[1]
    depth = embed_ref.shape[1]
    glob = w_ref[:, :, :, :, w_ref.shape[-1] - depth:].reshape(width, depth)
    out_ref[...] = lax.dot_general(embed_ref[...], glob, (((1,), (1,)), ((), ())),
                                   preferred_element_type=jnp.float32).astype(jnp.bfloat16)


def add_call(embeds, weights, width):
    vmem = pl.BlockSpec(memory_space=pltpu.VMEM)
    return pl.pallas_call(
        add_body,
        out_shape=jax.ShapeDtypeStruct((embeds.shape[0], width), jnp.bfloat16),
        in_specs=[vmem, vmem], out_specs=vmem,
        compiler_params=pltpu.CompilerParams(vmem_limit_bytes=24 * 2 ** 20),
        name="global_add",
    )(embeds, weights)


def attend(q, k, v, seen, head_of):
    rows, lanes = q.shape
    in_group = lanes // HEAD_DIM
    zero = jnp.zeros_like(q)
    spread = jnp.concatenate([jnp.where(head_of == j, q, zero) for j in range(in_group)], axis=0)
    scores = lax.dot_general(spread, k, (((1,), (1,)), ((), ())),
                             preferred_element_type=jnp.float32) * HEAD_DIM ** (-0.5)
    scores = jnp.where(seen, scores, -1e30)
    e = jnp.exp(scores - jnp.max(scores, axis=-1, keepdims=True))
    attn = (e / jnp.sum(e, axis=-1, keepdims=True)).astype(jnp.bfloat16)
    wide = jnp.dot(attn, v, preferred_element_type=jnp.float32)
    ctx = wide[:rows]
    for j in range(1, in_group):
        ctx = jnp.where(head_of == j, wide[j * rows:(j + 1) * rows], ctx)
    return ctx.astype(jnp.bfloat16)


def layer_body(final, t_ref, meta_ref, recv_ref, embed_ref, add_ref, gain_ref, final_gain_ref,
               w_ref, *rest):
    if final:
        out_ref, logits_ref, ctx_buf, normed_buf, proj_buf = rest
    else:
        out_ref, ctx_buf, normed_buf, proj_buf = rest
    rows, width = out_ref.shape
    lanes = width // GROUPS
    micro_count = add_ref.shape[0]
    section = meta_ref[0]
    last_section = meta_ref[1]
    micro = t_ref[0] - 2 * section
    active = (micro >= 0) & (micro < micro_count)

    @pl.when(active)
    def _():
        x = jnp.where(section == 0, embed_ref[micro], recv_ref[...])
        hidden = x.astype(jnp.float32) + add_ref[micro].astype(jnp.float32)
        normed = norm_rows(hidden, gain_ref[...])
        row = lax.broadcasted_iota(jnp.int32, (rows, rows), 0)
        col = lax.broadcasted_iota(jnp.int32, (rows, rows), 1)
        seen = (row // PATCH == col // PATCH) & (col <= row)
        seen = jnp.concatenate([seen] * (lanes // HEAD_DIM), axis=0)
        head_of = lax.broadcasted_iota(jnp.int32, (rows, lanes), 1) // HEAD_DIM

        def project(step, _):
            for k in range(GROUPS // PROJECT_STEPS):
                g = step * (GROUPS // PROJECT_STEPS) + k
                for p in range(3):
                    at = p * width + g * lanes
                    if PROJECT_STEPS > 1:
                        at = pl.multiple_of(at, lanes)
                    w = w_ref[:, :, :, :, pl.ds(at, lanes)].reshape(width, lanes)
                    proj = jnp.dot(normed_buf[...], w, preferred_element_type=jnp.float32)
                    proj_buf[p, g] = proj.astype(jnp.bfloat16)
            return 0

        def attention(step, _):
            for k in range(GROUPS // ATTEND_STEPS):
                g = step * (GROUPS // ATTEND_STEPS) + k
                at = g * lanes
                if ATTEND_STEPS > 1:
                    at = pl.multiple_of(at, lanes)
                ctx = attend(proj_buf[0, g], proj_buf[1, g], proj_buf[2, g], seen, head_of)
                ctx_buf[:, pl.ds(at, lanes)] = ctx
            return 0

        def run(steps, body):
            if steps > 1:
                lax.fori_loop(0, steps, body, 0)
            else:
                body(0, 0)

        normed_buf[...] = normed
        run(PROJECT_STEPS, project)
        run(ATTEND_STEPS, attention)
        mixed = jnp.dot(ctx_buf[...], w_ref[:, :, :, :, 3 * width:4 * width].reshape(width, width),
                        preferred_element_type=jnp.float32)
        out_ref[...] = (hidden + mixed).astype(jnp.bfloat16)
        if final:
            @pl.when(section == last_section)
            def _():
                final_rows = norm_rows(out_ref[...].astype(jnp.float32), final_gain_ref[...])
                scores = jnp.dot(final_rows, w_ref[:, :, :, :, 4 * width:4 * width + VOCAB].reshape(width, VOCAB),
                                 preferred_element_type=jnp.float32)
                patch = meta_ref[2] + lax.broadcasted_iota(jnp.int32, scores.shape, 0) // PATCH
                live = patch < meta_ref[3 + micro]
                logits_ref[...] = jnp.where(live, scores, 0.0).astype(jnp.bfloat16)


def layer_call(t, meta, recv, embeds, adds, gain, final_gain, weights, final):
    rows, width = recv.shape
    vmem = pl.BlockSpec(memory_space=pltpu.VMEM)
    smem = pl.BlockSpec(memory_space=pltpu.SMEM)
    x_shape = jax.ShapeDtypeStruct((rows, width), jnp.bfloat16)
    scratch = [
        pltpu.VMEM((rows, width), jnp.bfloat16),
        pltpu.VMEM((rows, width), jnp.bfloat16),
        pltpu.VMEM((3, GROUPS, rows, width // GROUPS), jnp.bfloat16),
    ]
    out_shape = [x_shape] + ([jax.ShapeDtypeStruct((rows, VOCAB), jnp.bfloat16)] if final else [])
    return pl.pallas_call(
        functools.partial(layer_body, final),
        out_shape=out_shape,
        in_specs=[smem, smem] + [vmem] * 6,
        out_specs=[vmem] * len(out_shape),
        scratch_shapes=scratch,
        compiler_params=pltpu.CompilerParams(vmem_limit_bytes=8 * 2 ** 20),
        cost_estimate=pl.CostEstimate(flops=8 * rows * width * width, bytes_accessed=8 * width * width,
                                      transcendentals=rows * rows * 16),
        name="layer_final" if final else "layer",
    )(t, meta, recv, embeds, adds, gain, final_gain, weights)


def previous_bytes(byte_ids):
    blocks = byte_ids.reshape(-1, PATCH)
    shifted = jnp.concatenate([jnp.zeros((blocks.shape[0], 1), jnp.int32), blocks[:, :-1]], axis=1)
    return shifted.reshape(-1)


def shards(tokens, doc_patches, global_embed, byte_table, w_qkv, w_out, layer_gain, w_global,
           final_gain, w_head):
    sections = lax.axis_size("section")
    columns = lax.axis_size("dp")
    section = lax.axis_index("section")
    column = lax.axis_index("dp")
    micro_count, row_count = tokens.shape
    width = byte_table.shape[1]

    own = jnp.concatenate([w_qkv[0], w_out[0], w_head.T, w_global.T], axis=1)
    pieces, near = gather_plane(own)

    copies = jnp.broadcast_to(global_embed, (sections, *global_embed.shape[1:]))
    copies, _ = lax.optimization_barrier((copies, near))
    globals_ = lax.all_to_all(copies, "section", split_axis=0, concat_axis=0, tiled=True)
    globals_ = globals_.reshape(micro_count * row_count, -1)

    place = jnp.stack([column // (X_SIZE * Z_SIZE), column // Z_SIZE % X_SIZE, column % Z_SIZE]).astype(jnp.int32)
    weights = pack_call(place, pieces)

    byte_ids = previous_bytes(tokens.reshape(-1))
    one_hot = (byte_ids[:, None] == jnp.arange(byte_table.shape[0], dtype=jnp.int32)[None, :]).astype(jnp.bfloat16)
    embeds = jnp.dot(one_hot, byte_table, preferred_element_type=jnp.float32).astype(jnp.bfloat16)
    embeds = embeds.reshape(micro_count, row_count, width)
    adds = add_call(globals_, weights, width).reshape(micro_count, row_count, width)

    meta = jnp.concatenate([
        jnp.stack([section, jnp.int32(sections - 1), column * (row_count // PATCH)]).astype(jnp.int32),
        doc_patches])
    final_gain = final_gain.reshape(1, width)

    def send(t, block):
        onward = [(s, s + 1) for s in range(sections - 1) if 0 <= t - 2 * s < micro_count]
        return lax.ppermute(block, "section", onward)

    fill = 2 * (sections - 1)
    steps = fill + micro_count
    arrived = jnp.zeros((row_count, width), jnp.bfloat16)
    sent = piece = total = None
    for t in range(steps):
        coming = send(t - 1, sent) if 0 < t < steps - 1 else arrived
        if piece is not None:
            arrived, piece = lax.optimization_barrier((arrived, piece))
            total = piece if total is None else total + piece
            piece = None
        final = t >= fill
        got = layer_call(jnp.full((1,), t, jnp.int32), meta, arrived, embeds, adds, layer_gain, final_gain, weights, final)
        if final:
            micro = t - fill
            logits = got[1]
            if micro == sections - 1:
                total = total + jnp.where(section == micro, logits, jnp.zeros_like(logits))
            else:
                piece = lax.ppermute(logits, "section", [(sections - 1, micro)])
        sent, arrived = got[0], coming
    return total[None]


def solution(mesh):
    in_specs = (
        P(None, "dp"), P(), P("section", "dp", None), P(), P("section", "dp", None),
        P("section", "dp", None), P("section", None), P(None, "dp"), P(), P(None, "dp"),
    )
    return jax.shard_map(shards, mesh=mesh, in_specs=in_specs, out_specs=P("section", "dp", None), check_vma=False)
```

```python
import functools

import jax
import jax.numpy as jnp
from jax import lax
from jax.experimental import pallas as pl
from jax.experimental.pallas import tpu as pltpu
from jax.sharding import PartitionSpec as P


PATCH = 8
HEAD_DIM = 64
GROUPS = 4
X_SIZE, Z_SIZE = 4, 8
SHARD = 16
VOCAB = 256


def norm_rows(hidden, gain):
    scale = lax.rsqrt(jnp.mean(hidden * hidden, axis=-1, keepdims=True) + 1e-06)
    return (hidden * scale * gain.astype(jnp.float32)).astype(jnp.bfloat16)


def pack_body(place_ref, *refs):
    half, x, z = place_ref[0], place_ref[1], place_ref[2]
    near, ups, downs, up_far, down_far = refs[0], refs[1:4], refs[4:7], refs[7], refs[8]
    cross, cross_up, cross_down, cross_far_a, cross_far_b = refs[9:14]
    out_ref, sems = refs[14:]
    copies = []

    def move(source, target):
        copy = pltpu.make_async_copy(source, target, sems.at[len(copies)])
        copy.start()
        copies.append(copy)

    def at_z(step):
        return lax.rem(z + step + Z_SIZE, Z_SIZE)

    def at_x(step):
        return lax.rem(x + step + X_SIZE, X_SIZE)

    move(near, out_ref.at[half, :, z])
    for i in range(3):
        move(ups[i], out_ref.at[half, :, at_z(-1 - i)])
        move(downs[i], out_ref.at[half, :, at_z(1 + i)])
    middle = X_SIZE // 2
    move(up_far, out_ref.at[half, pl.ds(0, middle), at_z(4)])
    move(down_far, out_ref.at[half, pl.ds(middle, middle), at_z(4)])
    middle = Z_SIZE // 2
    move(cross, out_ref.at[1 - half, x])
    move(cross_up, out_ref.at[1 - half, at_x(-1)])
    move(cross_down, out_ref.at[1 - half, at_x(1)])
    move(cross_far_a, out_ref.at[1 - half, at_x(2), pl.ds(0, middle)])
    move(cross_far_b, out_ref.at[1 - half, at_x(2), pl.ds(middle, middle)])
    for copy in copies:
        copy.wait()


def pack_call(place, pieces):
    columns = pieces[0].shape[-1]
    return pl.pallas_call(
        pack_body,
        out_shape=jax.ShapeDtypeStruct((2, X_SIZE, Z_SIZE, SHARD, columns), jnp.bfloat16),
        in_specs=[pl.BlockSpec(memory_space=pltpu.SMEM)] + [pl.BlockSpec(memory_space=pl.ANY)] * len(pieces),
        out_specs=pl.BlockSpec(memory_space=pltpu.VMEM),
        scratch_shapes=[pltpu.SemaphoreType.DMA((len(pieces),))],
        compiler_params=pltpu.CompilerParams(vmem_limit_bytes=16 * 2 ** 20),
        name="pack",
    )(place, *pieces)


def neighbours(axis, step):
    pairs = []
    for h in range(2):
        for x in range(X_SIZE):
            for z in range(Z_SIZE):
                to_h, to_x, to_z = h, x, z
                if axis == "y":
                    to_h = (h + step) % 2
                elif axis == "x":
                    to_x = (x + step) % X_SIZE
                else:
                    to_z = (z + step) % Z_SIZE
                pairs.append(((h * X_SIZE + x) * Z_SIZE + z, (to_h * X_SIZE + to_x) * Z_SIZE + to_z))
    return pairs


def to_team(shard, teams):
    copies = jnp.broadcast_to(shard, (len(teams[0]), *shard.shape))
    return lax.all_to_all(copies, "dp", split_axis=0, concat_axis=0, axis_index_groups=teams, tiled=True)


def gather_plane(own):
    def shift(block, axis, step):
        return lax.ppermute(block, "dp", neighbours(axis, step))

    along_x = [[(h * X_SIZE + x) * Z_SIZE + z for x in range(X_SIZE)] for h in range(2) for z in range(Z_SIZE)]
    along_z = [[r * Z_SIZE + z for z in range(Z_SIZE)] for r in range(2 * X_SIZE)]
    other = shift(own, "y", 1)
    near = to_team(own, along_x)
    ups, downs = [near], [near]
    for _ in range(3):
        ups.append(shift(ups[-1], "z", 1))
        downs.append(shift(downs[-1], "z", -1))
    up_far = shift(ups[-1][:X_SIZE // 2], "z", 1)
    down_far = shift(downs[-1][X_SIZE // 2:], "z", -1)
    cross = to_team(other, along_z)
    cross_up = shift(cross, "x", 1)
    cross_down = shift(cross, "x", -1)
    far_a = shift(cross_up[:Z_SIZE // 2], "x", 1)
    far_b = shift(cross_down[Z_SIZE // 2:], "x", -1)
    pieces = [near, *ups[1:], *downs[1:], up_far, down_far, cross, cross_up, cross_down, far_a, far_b]
    return pieces, other


def add_body(embed_ref, w_ref, out_ref):
    width = out_ref.shape[1]
    depth = embed_ref.shape[1]
    glob = w_ref[:, :, :, :, w_ref.shape[-1] - depth:].reshape(width, depth)
    out_ref[...] = lax.dot_general(embed_ref[...], glob, (((1,), (1,)), ((), ())),
                                   preferred_element_type=jnp.float32).astype(jnp.bfloat16)


def add_call(embeds, weights, width):
    vmem = pl.BlockSpec(memory_space=pltpu.VMEM)
    return pl.pallas_call(
        add_body,
        out_shape=jax.ShapeDtypeStruct((embeds.shape[0], width), jnp.bfloat16),
        in_specs=[vmem, vmem], out_specs=vmem,
        compiler_params=pltpu.CompilerParams(vmem_limit_bytes=24 * 2 ** 20),
        name="global_add",
    )(embeds, weights)


def attend(q, k, v, seen, head_of):
    rows, lanes = q.shape
    in_group = lanes // HEAD_DIM
    zero = jnp.zeros_like(q)
    spread = jnp.concatenate([jnp.where(head_of == j, q, zero) for j in range(in_group)], axis=0)
    scores = lax.dot_general(spread, k, (((1,), (1,)), ((), ())),
                             preferred_element_type=jnp.float32) * HEAD_DIM ** (-0.5)
    scores = jnp.where(seen, scores, -1e30)
    e = jnp.exp(scores - jnp.max(scores, axis=-1, keepdims=True))
    attn = (e / jnp.sum(e, axis=-1, keepdims=True)).astype(jnp.bfloat16)
    wide = jnp.dot(attn, v, preferred_element_type=jnp.float32)
    ctx = wide[:rows]
    for j in range(1, in_group):
        ctx = jnp.where(head_of == j, wide[j * rows:(j + 1) * rows], ctx)
    return ctx.astype(jnp.bfloat16)


def layer_body(final, t_ref, meta_ref, recv_ref, embed_ref, add_ref, gain_ref, final_gain_ref,
               w_ref, *rest):
    if final:
        out_ref, logits_ref, ctx_buf = rest
    else:
        out_ref, ctx_buf = rest
    rows, width = out_ref.shape
    lanes = width // GROUPS
    micro_count = add_ref.shape[0]
    section = meta_ref[0]
    last_section = meta_ref[1]
    micro = t_ref[0] - 2 * section
    active = (micro >= 0) & (micro < micro_count)
    if final:
        @pl.when(section != last_section)
        def _():
            logits_ref[...] = jnp.zeros_like(logits_ref)

    @pl.when(active)
    def _():
        x = jnp.where(section == 0, embed_ref[micro], recv_ref[...])
        hidden = x.astype(jnp.float32) + add_ref[micro].astype(jnp.float32)
        normed = norm_rows(hidden, gain_ref[...])
        row = lax.broadcasted_iota(jnp.int32, (rows, rows), 0)
        col = lax.broadcasted_iota(jnp.int32, (rows, rows), 1)
        seen = (row // PATCH == col // PATCH) & (col <= row)
        seen = jnp.concatenate([seen] * (lanes // HEAD_DIM), axis=0)
        head_of = lax.broadcasted_iota(jnp.int32, (rows, lanes), 1) // HEAD_DIM

        def project(at):
            w = w_ref[:, :, :, :, at:at + lanes].reshape(width, lanes)
            return jnp.dot(normed, w, preferred_element_type=jnp.float32).astype(jnp.bfloat16)

        projs = [[project(p * width + g * lanes) for p in range(3)] for g in range(GROUPS)]
        for g in range(GROUPS):
            ctx_buf[:, g * lanes:(g + 1) * lanes] = attend(*projs[g], seen, head_of)
        mixed = jnp.dot(ctx_buf[...], w_ref[:, :, :, :, 3 * width:4 * width].reshape(width, width),
                        preferred_element_type=jnp.float32)
        out_ref[...] = (hidden + mixed).astype(jnp.bfloat16)
        if final:
            @pl.when(section == last_section)
            def _():
                final_rows = norm_rows(out_ref[...].astype(jnp.float32), final_gain_ref[...])
                scores = jnp.dot(final_rows, w_ref[:, :, :, :, 4 * width:4 * width + VOCAB].reshape(width, VOCAB),
                                 preferred_element_type=jnp.float32)
                patch = meta_ref[2] + lax.broadcasted_iota(jnp.int32, scores.shape, 0) // PATCH
                live = patch < meta_ref[3 + micro]
                logits_ref[...] = jnp.where(live, scores, 0.0).astype(jnp.bfloat16)


def layer_call(t, meta, recv, embeds, adds, gain, final_gain, weights, final):
    rows, width = recv.shape
    vmem = pl.BlockSpec(memory_space=pltpu.VMEM)
    smem = pl.BlockSpec(memory_space=pltpu.SMEM)
    x_shape = jax.ShapeDtypeStruct((rows, width), jnp.bfloat16)
    scratch = [pltpu.VMEM((rows, width), jnp.bfloat16)]
    out_shape = [x_shape] + ([jax.ShapeDtypeStruct((rows, VOCAB), jnp.bfloat16)] if final else [])
    return pl.pallas_call(
        functools.partial(layer_body, final),
        out_shape=out_shape,
        in_specs=[smem, smem] + [vmem] * 6,
        out_specs=[vmem] * len(out_shape),
        scratch_shapes=scratch,
        compiler_params=pltpu.CompilerParams(vmem_limit_bytes=8 * 2 ** 20),
        cost_estimate=pl.CostEstimate(flops=8 * rows * width * width, bytes_accessed=8 * width * width,
                                      transcendentals=rows * rows * 16),
        name="layer_final" if final else "layer",
    )(t, meta, recv, embeds, adds, gain, final_gain, weights)


def previous_bytes(byte_ids):
    blocks = byte_ids.reshape(-1, PATCH)
    shifted = jnp.concatenate([jnp.zeros((blocks.shape[0], 1), jnp.int32), blocks[:, :-1]], axis=1)
    return shifted.reshape(-1)


def shards(tokens, doc_patches, global_embed, byte_table, w_qkv, w_out, layer_gain, w_global,
           final_gain, w_head):
    sections = lax.axis_size("section")
    section = lax.axis_index("section")
    column = lax.axis_index("dp")
    micro_count, row_count = tokens.shape
    width = byte_table.shape[1]

    own = jnp.concatenate([w_qkv[0], w_out[0], w_head.T, w_global.T], axis=1)
    pieces, other = gather_plane(own)

    copies = jnp.broadcast_to(global_embed, (sections, *global_embed.shape[1:]))
    copies, _ = lax.optimization_barrier((copies, other))
    globals_ = lax.all_to_all(copies, "section", split_axis=0, concat_axis=0, tiled=True)
    globals_ = globals_.reshape(micro_count * row_count, -1)

    place = jnp.stack([column // (X_SIZE * Z_SIZE), column // Z_SIZE % X_SIZE, column % Z_SIZE]).astype(jnp.int32)
    weights = pack_call(place, pieces)

    byte_ids = previous_bytes(tokens.reshape(-1))
    one_hot = (byte_ids[:, None] == jnp.arange(byte_table.shape[0], dtype=jnp.int32)[None, :]).astype(jnp.bfloat16)
    embeds = jnp.dot(one_hot, byte_table, preferred_element_type=jnp.float32).astype(jnp.bfloat16)
    embeds = embeds.reshape(micro_count, row_count, width)
    adds = add_call(globals_, weights, width).reshape(micro_count, row_count, width)

    meta = jnp.concatenate([
        jnp.stack([section, jnp.int32(sections - 1), column * (row_count // PATCH)]).astype(jnp.int32),
        doc_patches])
    final_gain = final_gain.reshape(1, width)

    def send(t, block):
        onward = [(s, s + 1) for s in range(sections - 1) if 0 <= t - 2 * s < micro_count]
        return lax.ppermute(block, "section", onward)

    fill = 2 * (sections - 1)
    steps = fill + micro_count
    arrived = jnp.zeros((row_count, width), jnp.bfloat16)
    sent = None
    pieces = []
    for t in range(steps):
        coming = send(t - 1, sent) if 0 < t < steps - 1 else arrived
        if t - fill >= 2:
            arrived, pieces[t - fill - 2] = lax.optimization_barrier((arrived, pieces[t - fill - 2]))
        final = t >= fill
        got = layer_call(jnp.full((1,), t, jnp.int32), meta, arrived, embeds, adds, layer_gain, final_gain, weights, final)
        if final:
            micro = t - fill
            pieces.append(got[1] if micro == sections - 1 else lax.ppermute(got[1], "section", [(sections - 1, micro)]))
        sent, arrived = got[0], coming
    total = sum(pieces[1:], pieces[0])
    return total[None]


def solution(mesh):
    in_specs = (
        P(None, "dp"), P(), P("section", "dp", None), P(), P("section", "dp", None),
        P("section", "dp", None), P("section", None), P(None, "dp"), P(), P(None, "dp"),
    )
    return jax.shard_map(shards, mesh=mesh, in_specs=in_specs, out_specs=P("section", "dp", None), check_vma=False)
```

```python
import functools

import jax
import jax.numpy as jnp
from jax import lax
from jax.experimental import pallas as pl
from jax.experimental.pallas import tpu as pltpu
from jax.sharding import PartitionSpec as P


PATCH = 8
HEAD_DIM = 64
GROUPS = 4
X_SIZE, Z_SIZE = 4, 8
SHARD = 16
VOCAB = 256


def norm_rows(hidden, gain):
    scale = lax.rsqrt(jnp.mean(hidden * hidden, axis=-1, keepdims=True) + 1e-06)
    return (hidden * scale * gain.astype(jnp.float32)).astype(jnp.bfloat16)


X_FROM = (0, -1, 1, 2)


def pack_body(place_ref, *refs):
    half, x, z = place_ref[0], place_ref[1], place_ref[2]
    near, ups, downs, up_far, down_far = refs[0], refs[1:4], refs[4:7], refs[7], refs[8]
    cross, cross_up, cross_down, cross_far_a, cross_far_b = refs[9:14]
    out_ref, sems = refs[14:]
    copies = []

    def move(source, target):
        copy = pltpu.make_async_copy(source, target, sems.at[len(copies)])
        copy.start()
        copies.append(copy)

    def at_z(step):
        return lax.rem(z + step + Z_SIZE, Z_SIZE)

    def at_x(step):
        return lax.rem(x + step + X_SIZE, X_SIZE)

    def move_columns(ref, step, first=0):
        for k in range(ref.shape[0]):
            move(ref.at[k], out_ref.at[half, at_x(X_FROM[first + k]), at_z(step)])

    move_columns(near, 0)
    for i in range(3):
        move_columns(ups[i], -1 - i)
        move_columns(downs[i], 1 + i)
    move_columns(up_far, 4)
    move_columns(down_far, 4, X_SIZE // 2)
    middle = Z_SIZE // 2
    move(cross, out_ref.at[1 - half, x])
    move(cross_up, out_ref.at[1 - half, at_x(-1)])
    move(cross_down, out_ref.at[1 - half, at_x(1)])
    move(cross_far_a, out_ref.at[1 - half, at_x(2), pl.ds(0, middle)])
    move(cross_far_b, out_ref.at[1 - half, at_x(2), pl.ds(middle, middle)])
    for copy in copies:
        copy.wait()


def pack_call(place, pieces):
    columns = pieces[0].shape[-1]
    return pl.pallas_call(
        pack_body,
        out_shape=jax.ShapeDtypeStruct((2, X_SIZE, Z_SIZE, SHARD, columns), jnp.bfloat16),
        in_specs=[pl.BlockSpec(memory_space=pltpu.SMEM)] + [pl.BlockSpec(memory_space=pl.ANY)] * len(pieces),
        out_specs=pl.BlockSpec(memory_space=pltpu.VMEM),
        scratch_shapes=[pltpu.SemaphoreType.DMA((X_SIZE * Z_SIZE + 5,))],
        compiler_params=pltpu.CompilerParams(vmem_limit_bytes=16 * 2 ** 20),
        name="pack",
    )(place, *pieces)


def neighbours(axis, step):
    pairs = []
    for h in range(2):
        for x in range(X_SIZE):
            for z in range(Z_SIZE):
                to_h, to_x, to_z = h, x, z
                if axis == "y":
                    to_h = (h + step) % 2
                elif axis == "x":
                    to_x = (x + step) % X_SIZE
                else:
                    to_z = (z + step) % Z_SIZE
                pairs.append(((h * X_SIZE + x) * Z_SIZE + z, (to_h * X_SIZE + to_x) * Z_SIZE + to_z))
    return pairs


def to_team(shard, teams):
    copies = jnp.broadcast_to(shard, (len(teams[0]), *shard.shape))
    return lax.all_to_all(copies, "dp", split_axis=0, concat_axis=0, axis_index_groups=teams, tiled=True)


def gather_plane(own):
    def shift(block, axis, step):
        return lax.ppermute(block, "dp", neighbours(axis, step))

    along_z = [[r * Z_SIZE + z for z in range(Z_SIZE)] for r in range(2 * X_SIZE)]
    other = shift(own, "y", 1)
    near = jnp.stack([own, shift(own, "x", 1), shift(own, "x", -1), shift(own, "x", 2)])
    ups, downs = [near], [near]
    for _ in range(3):
        ups.append(shift(ups[-1], "z", 1))
        downs.append(shift(downs[-1], "z", -1))
    up_far = shift(ups[-1][:X_SIZE // 2], "z", 1)
    down_far = shift(downs[-1][X_SIZE // 2:], "z", -1)
    cross = to_team(other, along_z)
    cross_up = shift(cross, "x", 1)
    cross_down = shift(cross, "x", -1)
    far_a = shift(cross_up[:Z_SIZE // 2], "x", 1)
    far_b = shift(cross_down[Z_SIZE // 2:], "x", -1)
    pieces = [near, *ups[1:], *downs[1:], up_far, down_far, cross, cross_up, cross_down, far_a, far_b]
    return pieces, near


def add_body(embed_ref, w_ref, out_ref):
    width = out_ref.shape[1]
    depth = embed_ref.shape[1]
    glob = w_ref[:, :, :, :, w_ref.shape[-1] - depth:].reshape(width, depth)
    out_ref[...] = lax.dot_general(embed_ref[...], glob, (((1,), (1,)), ((), ())),
                                   preferred_element_type=jnp.float32).astype(jnp.bfloat16)


def add_call(embeds, weights, width):
    vmem = pl.BlockSpec(memory_space=pltpu.VMEM)
    return pl.pallas_call(
        add_body,
        out_shape=jax.ShapeDtypeStruct((embeds.shape[0], width), jnp.bfloat16),
        in_specs=[vmem, vmem], out_specs=vmem,
        compiler_params=pltpu.CompilerParams(vmem_limit_bytes=24 * 2 ** 20),
        name="global_add",
    )(embeds, weights)


def attend(q, k, v, seen, head_of):
    rows, lanes = q.shape
    in_group = lanes // HEAD_DIM
    zero = jnp.zeros_like(q)
    spread = jnp.concatenate([jnp.where(head_of == j, q, zero) for j in range(in_group)], axis=0)
    scores = lax.dot_general(spread, k, (((1,), (1,)), ((), ())),
                             preferred_element_type=jnp.float32) * HEAD_DIM ** (-0.5)
    scores = jnp.where(seen, scores, -1e30)
    e = jnp.exp(scores - jnp.max(scores, axis=-1, keepdims=True))
    attn = (e / jnp.sum(e, axis=-1, keepdims=True)).astype(jnp.bfloat16)
    wide = jnp.dot(attn, v, preferred_element_type=jnp.float32)
    ctx = wide[:rows]
    for j in range(1, in_group):
        ctx = jnp.where(head_of == j, wide[j * rows:(j + 1) * rows], ctx)
    return ctx.astype(jnp.bfloat16)


def layer_body(final, t_ref, meta_ref, recv_ref, embed_ref, add_ref, gain_ref, final_gain_ref,
               w_ref, *rest):
    if final:
        out_ref, logits_ref, ctx_buf = rest
    else:
        out_ref, ctx_buf = rest
    rows, width = out_ref.shape
    lanes = width // GROUPS
    micro_count = add_ref.shape[0]
    section = meta_ref[0]
    last_section = meta_ref[1]
    micro = t_ref[0] - 2 * section
    active = (micro >= 0) & (micro < micro_count)
    if final:
        @pl.when(section != last_section)
        def _():
            logits_ref[...] = jnp.zeros_like(logits_ref)

    @pl.when(active)
    def _():
        x = jnp.where(section == 0, embed_ref[micro], recv_ref[...])
        hidden = x.astype(jnp.float32) + add_ref[micro].astype(jnp.float32)
        normed = norm_rows(hidden, gain_ref[...])
        row = lax.broadcasted_iota(jnp.int32, (rows, rows), 0)
        col = lax.broadcasted_iota(jnp.int32, (rows, rows), 1)
        seen = (row // PATCH == col // PATCH) & (col <= row)
        seen = jnp.concatenate([seen] * (lanes // HEAD_DIM), axis=0)
        head_of = lax.broadcasted_iota(jnp.int32, (rows, lanes), 1) // HEAD_DIM

        def project(at):
            w = w_ref[:, :, :, :, at:at + lanes].reshape(width, lanes)
            return jnp.dot(normed, w, preferred_element_type=jnp.float32).astype(jnp.bfloat16)

        projs = [[project(p * width + g * lanes) for p in range(3)] for g in range(GROUPS)]
        for g in range(GROUPS):
            ctx_buf[:, g * lanes:(g + 1) * lanes] = attend(*projs[g], seen, head_of)
        mixed = jnp.dot(ctx_buf[...], w_ref[:, :, :, :, 3 * width:4 * width].reshape(width, width),
                        preferred_element_type=jnp.float32)
        out_ref[...] = (hidden + mixed).astype(jnp.bfloat16)
        if final:
            @pl.when(section == last_section)
            def _():
                final_rows = norm_rows(out_ref[...].astype(jnp.float32), final_gain_ref[...])
                scores = jnp.dot(final_rows, w_ref[:, :, :, :, 4 * width:4 * width + VOCAB].reshape(width, VOCAB),
                                 preferred_element_type=jnp.float32)
                patch = meta_ref[2] + lax.broadcasted_iota(jnp.int32, scores.shape, 0) // PATCH
                live = patch < meta_ref[3 + micro]
                logits_ref[...] = jnp.where(live, scores, 0.0).astype(jnp.bfloat16)


def layer_call(t, meta, recv, embeds, adds, gain, final_gain, weights, final):
    rows, width = recv.shape
    vmem = pl.BlockSpec(memory_space=pltpu.VMEM)
    smem = pl.BlockSpec(memory_space=pltpu.SMEM)
    x_shape = jax.ShapeDtypeStruct((rows, width), jnp.bfloat16)
    scratch = [pltpu.VMEM((rows, width), jnp.bfloat16)]
    out_shape = [x_shape] + ([jax.ShapeDtypeStruct((rows, VOCAB), jnp.bfloat16)] if final else [])
    return pl.pallas_call(
        functools.partial(layer_body, final),
        out_shape=out_shape,
        in_specs=[smem, smem] + [vmem] * 6,
        out_specs=[vmem] * len(out_shape),
        scratch_shapes=scratch,
        compiler_params=pltpu.CompilerParams(vmem_limit_bytes=8 * 2 ** 20),
        cost_estimate=pl.CostEstimate(flops=8 * rows * width * width, bytes_accessed=8 * width * width,
                                      transcendentals=rows * rows * 16),
        name="layer_final" if final else "layer",
    )(t, meta, recv, embeds, adds, gain, final_gain, weights)


def previous_bytes(byte_ids):
    blocks = byte_ids.reshape(-1, PATCH)
    shifted = jnp.concatenate([jnp.zeros((blocks.shape[0], 1), jnp.int32), blocks[:, :-1]], axis=1)
    return shifted.reshape(-1)


def shards(tokens, doc_patches, global_embed, byte_table, w_qkv, w_out, layer_gain, w_global,
           final_gain, w_head):
    sections = lax.axis_size("section")
    section = lax.axis_index("section")
    column = lax.axis_index("dp")
    micro_count, row_count = tokens.shape
    width = byte_table.shape[1]

    own = jnp.concatenate([w_qkv[0], w_out[0], w_head.T, w_global.T], axis=1)
    pieces, near = gather_plane(own)

    copies = jnp.broadcast_to(global_embed, (sections, *global_embed.shape[1:]))
    copies, _ = lax.optimization_barrier((copies, near))
    globals_ = lax.all_to_all(copies, "section", split_axis=0, concat_axis=0, tiled=True)
    globals_ = globals_.reshape(micro_count * row_count, -1)

    place = jnp.stack([column // (X_SIZE * Z_SIZE), column // Z_SIZE % X_SIZE, column % Z_SIZE]).astype(jnp.int32)
    weights = pack_call(place, pieces)

    byte_ids = previous_bytes(tokens.reshape(-1))
    one_hot = (byte_ids[:, None] == jnp.arange(byte_table.shape[0], dtype=jnp.int32)[None, :]).astype(jnp.bfloat16)
    embeds = jnp.dot(one_hot, byte_table, preferred_element_type=jnp.float32).astype(jnp.bfloat16)
    embeds = embeds.reshape(micro_count, row_count, width)
    adds = add_call(globals_, weights, width).reshape(micro_count, row_count, width)

    meta = jnp.concatenate([
        jnp.stack([section, jnp.int32(sections - 1), column * (row_count // PATCH)]).astype(jnp.int32),
        doc_patches])
    final_gain = final_gain.reshape(1, width)

    def send(t, block):
        onward = [(s, s + 1) for s in range(sections - 1) if 0 <= t - 2 * s < micro_count]
        return lax.ppermute(block, "section", onward)

    fill = 2 * (sections - 1)
    steps = fill + micro_count
    arrived = jnp.zeros((row_count, width), jnp.bfloat16)
    sent = None
    pieces = []
    for t in range(steps):
        coming = send(t - 1, sent) if 0 < t < steps - 1 else arrived
        if t - fill >= 2:
            arrived, pieces[t - fill - 2] = lax.optimization_barrier((arrived, pieces[t - fill - 2]))
        final = t >= fill
        got = layer_call(jnp.full((1,), t, jnp.int32), meta, arrived, embeds, adds, layer_gain, final_gain, weights, final)
        if final:
            micro = t - fill
            pieces.append(got[1] if micro == sections - 1 else lax.ppermute(got[1], "section", [(sections - 1, micro)]))
        sent, arrived = got[0], coming
    total = sum(pieces[1:], pieces[0])
    return total[None]


def solution(mesh):
    in_specs = (
        P(None, "dp"), P(), P("section", "dp", None), P(), P("section", "dp", None),
        P("section", "dp", None), P("section", None), P(None, "dp"), P(), P(None, "dp"),
    )
    return jax.shard_map(shards, mesh=mesh, in_specs=in_specs, out_specs=P("section", "dp", None), check_vma=False)
```

```python
import functools

import jax
import jax.numpy as jnp
from jax import lax
from jax.experimental import pallas as pl
from jax.experimental.pallas import tpu as pltpu
from jax.sharding import PartitionSpec as P


PATCH = 8
HEAD_DIM = 64
GROUPS = 4
X_SIZE, Z_SIZE = 4, 8
SHARD = 16
VOCAB = 256


def norm_rows(hidden, gain):
    scale = lax.rsqrt(jnp.mean(hidden * hidden, axis=-1, keepdims=True) + 1e-06)
    return (hidden * scale * gain.astype(jnp.float32)).astype(jnp.bfloat16)


X_FROM = (0, -1, 1, 2)
Z_FROM = (0, -1, -2, -3, 1, 2, 3, 4)


def pack_body(place_ref, *refs):
    half, x, z = place_ref[0], place_ref[1], place_ref[2]
    near, ups, downs, up_far, down_far = refs[0], refs[1:4], refs[4:7], refs[7], refs[8]
    cross, cross_up, cross_down, cross_far_a, cross_far_b = refs[9:14]
    out_ref, sems = refs[14:]
    copies = []

    def move(source, target):
        copy = pltpu.make_async_copy(source, target, sems.at[len(copies)])
        copy.start()
        copies.append(copy)

    def at_z(step):
        return lax.rem(z + step + Z_SIZE, Z_SIZE)

    def at_x(step):
        return lax.rem(x + step + X_SIZE, X_SIZE)

    def move_columns(ref, step, first=0):
        for k in range(ref.shape[0]):
            move(ref.at[k], out_ref.at[half, at_x(X_FROM[first + k]), at_z(step)])

    move_columns(near, 0)
    for i in range(3):
        move_columns(ups[i], -1 - i)
        move_columns(downs[i], 1 + i)
    move_columns(up_far, 4)
    move_columns(down_far, 4, X_SIZE // 2)

    def move_rows(ref, step, first=0):
        for k in range(ref.shape[0]):
            move(ref.at[k], out_ref.at[1 - half, at_x(step), at_z(Z_FROM[first + k])])

    move_rows(cross, 0)
    move_rows(cross_up, -1)
    move_rows(cross_down, 1)
    move_rows(cross_far_a, 2)
    move_rows(cross_far_b, 2, Z_SIZE // 2)
    for copy in copies:
        copy.wait()


def pack_call(place, pieces):
    columns = pieces[0].shape[-1]
    return pl.pallas_call(
        pack_body,
        out_shape=jax.ShapeDtypeStruct((2, X_SIZE, Z_SIZE, SHARD, columns), jnp.bfloat16),
        in_specs=[pl.BlockSpec(memory_space=pltpu.SMEM)] + [pl.BlockSpec(memory_space=pl.ANY)] * len(pieces),
        out_specs=pl.BlockSpec(memory_space=pltpu.VMEM),
        scratch_shapes=[pltpu.SemaphoreType.DMA((2 * X_SIZE * Z_SIZE,))],
        compiler_params=pltpu.CompilerParams(vmem_limit_bytes=16 * 2 ** 20),
        name="pack",
    )(place, *pieces)


def neighbours(axis, step):
    pairs = []
    for h in range(2):
        for x in range(X_SIZE):
            for z in range(Z_SIZE):
                to_h, to_x, to_z = h, x, z
                if axis == "y":
                    to_h = (h + step) % 2
                elif axis == "x":
                    to_x = (x + step) % X_SIZE
                else:
                    to_z = (z + step) % Z_SIZE
                pairs.append(((h * X_SIZE + x) * Z_SIZE + z, (to_h * X_SIZE + to_x) * Z_SIZE + to_z))
    return pairs


def gather_plane(own):
    def shift(block, axis, step):
        return lax.ppermute(block, "dp", neighbours(axis, step))

    other = shift(own, "y", 1)
    near = jnp.stack([own, shift(own, "x", 1), shift(own, "x", -1), shift(own, "x", 2)])
    ups, downs = [near], [near]
    for _ in range(3):
        ups.append(shift(ups[-1], "z", 1))
        downs.append(shift(downs[-1], "z", -1))
    up_far = shift(ups[-1][:X_SIZE // 2], "z", 1)
    down_far = shift(downs[-1][X_SIZE // 2:], "z", -1)
    cross_ups, cross_downs = [other], [other]
    for i in range(4):
        if i < 3:
            cross_ups.append(shift(cross_ups[-1], "z", 1))
        cross_downs.append(shift(cross_downs[-1], "z", -1))
    cross = jnp.stack(cross_ups + cross_downs[1:])
    cross_up = shift(cross, "x", 1)
    cross_down = shift(cross, "x", -1)
    far_a = shift(cross_up[:Z_SIZE // 2], "x", 1)
    far_b = shift(cross_down[Z_SIZE // 2:], "x", -1)
    pieces = [near, *ups[1:], *downs[1:], up_far, down_far, cross, cross_up, cross_down, far_a, far_b]
    return pieces, near


def add_body(embed_ref, w_ref, out_ref):
    width = out_ref.shape[1]
    depth = embed_ref.shape[1]
    glob = w_ref[:, :, :, :, w_ref.shape[-1] - depth:].reshape(width, depth)
    out_ref[...] = lax.dot_general(embed_ref[...], glob, (((1,), (1,)), ((), ())),
                                   preferred_element_type=jnp.float32).astype(jnp.bfloat16)


def add_call(embeds, weights, width):
    vmem = pl.BlockSpec(memory_space=pltpu.VMEM)
    return pl.pallas_call(
        add_body,
        out_shape=jax.ShapeDtypeStruct((embeds.shape[0], width), jnp.bfloat16),
        in_specs=[vmem, vmem], out_specs=vmem,
        compiler_params=pltpu.CompilerParams(vmem_limit_bytes=24 * 2 ** 20),
        name="global_add",
    )(embeds, weights)


def attend(q, k, v, seen, head_of):
    rows, lanes = q.shape
    in_group = lanes // HEAD_DIM
    zero = jnp.zeros_like(q)
    spread = jnp.concatenate([jnp.where(head_of == j, q, zero) for j in range(in_group)], axis=0)
    scores = lax.dot_general(spread, k, (((1,), (1,)), ((), ())),
                             preferred_element_type=jnp.float32) * HEAD_DIM ** (-0.5)
    scores = jnp.where(seen, scores, -1e30)
    e = jnp.exp(scores - jnp.max(scores, axis=-1, keepdims=True))
    attn = (e / jnp.sum(e, axis=-1, keepdims=True)).astype(jnp.bfloat16)
    wide = jnp.dot(attn, v, preferred_element_type=jnp.float32)
    ctx = wide[:rows]
    for j in range(1, in_group):
        ctx = jnp.where(head_of == j, wide[j * rows:(j + 1) * rows], ctx)
    return ctx.astype(jnp.bfloat16)


def layer_body(final, t_ref, meta_ref, recv_ref, embed_ref, add_ref, gain_ref, final_gain_ref,
               w_ref, *rest):
    if final:
        out_ref, logits_ref, ctx_buf = rest
    else:
        out_ref, ctx_buf = rest
    rows, width = out_ref.shape
    lanes = width // GROUPS
    micro_count = add_ref.shape[0]
    section = meta_ref[0]
    last_section = meta_ref[1]
    micro = t_ref[0] - 2 * section
    active = (micro >= 0) & (micro < micro_count)
    if final:
        @pl.when(section != last_section)
        def _():
            logits_ref[...] = jnp.zeros_like(logits_ref)

    @pl.when(active)
    def _():
        x = jnp.where(section == 0, embed_ref[micro], recv_ref[...])
        hidden = x.astype(jnp.float32) + add_ref[micro].astype(jnp.float32)
        normed = norm_rows(hidden, gain_ref[...])
        row = lax.broadcasted_iota(jnp.int32, (rows, rows), 0)
        col = lax.broadcasted_iota(jnp.int32, (rows, rows), 1)
        seen = (row // PATCH == col // PATCH) & (col <= row)
        seen = jnp.concatenate([seen] * (lanes // HEAD_DIM), axis=0)
        head_of = lax.broadcasted_iota(jnp.int32, (rows, lanes), 1) // HEAD_DIM

        def project(at):
            w = w_ref[:, :, :, :, at:at + lanes].reshape(width, lanes)
            return jnp.dot(normed, w, preferred_element_type=jnp.float32).astype(jnp.bfloat16)

        projs = [[project(p * width + g * lanes) for p in range(3)] for g in range(GROUPS)]
        for g in range(GROUPS):
            ctx_buf[:, g * lanes:(g + 1) * lanes] = attend(*projs[g], seen, head_of)
        mixed = jnp.dot(ctx_buf[...], w_ref[:, :, :, :, 3 * width:4 * width].reshape(width, width),
                        preferred_element_type=jnp.float32)
        out_ref[...] = (hidden + mixed).astype(jnp.bfloat16)
        if final:
            @pl.when(section == last_section)
            def _():
                final_rows = norm_rows(out_ref[...].astype(jnp.float32), final_gain_ref[...])
                scores = jnp.dot(final_rows, w_ref[:, :, :, :, 4 * width:4 * width + VOCAB].reshape(width, VOCAB),
                                 preferred_element_type=jnp.float32)
                patch = meta_ref[2] + lax.broadcasted_iota(jnp.int32, scores.shape, 0) // PATCH
                live = patch < meta_ref[3 + micro]
                logits_ref[...] = jnp.where(live, scores, 0.0).astype(jnp.bfloat16)


def layer_call(t, meta, recv, embeds, adds, gain, final_gain, weights, final):
    rows, width = recv.shape
    vmem = pl.BlockSpec(memory_space=pltpu.VMEM)
    smem = pl.BlockSpec(memory_space=pltpu.SMEM)
    x_shape = jax.ShapeDtypeStruct((rows, width), jnp.bfloat16)
    scratch = [pltpu.VMEM((rows, width), jnp.bfloat16)]
    out_shape = [x_shape] + ([jax.ShapeDtypeStruct((rows, VOCAB), jnp.bfloat16)] if final else [])
    return pl.pallas_call(
        functools.partial(layer_body, final),
        out_shape=out_shape,
        in_specs=[smem, smem] + [vmem] * 6,
        out_specs=[vmem] * len(out_shape),
        scratch_shapes=scratch,
        compiler_params=pltpu.CompilerParams(vmem_limit_bytes=8 * 2 ** 20),
        cost_estimate=pl.CostEstimate(flops=8 * rows * width * width, bytes_accessed=8 * width * width,
                                      transcendentals=rows * rows * 16),
        name="layer_final" if final else "layer",
    )(t, meta, recv, embeds, adds, gain, final_gain, weights)


def previous_bytes(byte_ids):
    blocks = byte_ids.reshape(-1, PATCH)
    shifted = jnp.concatenate([jnp.zeros((blocks.shape[0], 1), jnp.int32), blocks[:, :-1]], axis=1)
    return shifted.reshape(-1)


def shards(tokens, doc_patches, global_embed, byte_table, w_qkv, w_out, layer_gain, w_global,
           final_gain, w_head):
    sections = lax.axis_size("section")
    section = lax.axis_index("section")
    column = lax.axis_index("dp")
    micro_count, row_count = tokens.shape
    width = byte_table.shape[1]

    own = jnp.concatenate([w_qkv[0], w_out[0], w_head.T, w_global.T], axis=1)
    pieces, near = gather_plane(own)

    copies = jnp.broadcast_to(global_embed, (sections, *global_embed.shape[1:]))
    copies, _ = lax.optimization_barrier((copies, near))
    globals_ = lax.all_to_all(copies, "section", split_axis=0, concat_axis=0, tiled=True)
    globals_ = globals_.reshape(micro_count * row_count, -1)

    place = jnp.stack([column // (X_SIZE * Z_SIZE), column // Z_SIZE % X_SIZE, column % Z_SIZE]).astype(jnp.int32)
    weights = pack_call(place, pieces)

    byte_ids = previous_bytes(tokens.reshape(-1))
    one_hot = (byte_ids[:, None] == jnp.arange(byte_table.shape[0], dtype=jnp.int32)[None, :]).astype(jnp.bfloat16)
    embeds = jnp.dot(one_hot, byte_table, preferred_element_type=jnp.float32).astype(jnp.bfloat16)
    embeds = embeds.reshape(micro_count, row_count, width)
    adds = add_call(globals_, weights, width).reshape(micro_count, row_count, width)

    meta = jnp.concatenate([
        jnp.stack([section, jnp.int32(sections - 1), column * (row_count // PATCH)]).astype(jnp.int32),
        doc_patches])
    final_gain = final_gain.reshape(1, width)

    def send(t, block):
        onward = [(s, s + 1) for s in range(sections - 1) if 0 <= t - 2 * s < micro_count]
        return lax.ppermute(block, "section", onward)

    fill = 2 * (sections - 1)
    steps = fill + micro_count
    arrived = jnp.zeros((row_count, width), jnp.bfloat16)
    sent = None
    pieces = []
    for t in range(steps):
        coming = send(t - 1, sent) if 0 < t < steps - 1 else arrived
        if t - fill >= 2:
            arrived, pieces[t - fill - 2] = lax.optimization_barrier((arrived, pieces[t - fill - 2]))
        final = t >= fill
        got = layer_call(jnp.full((1,), t, jnp.int32), meta, arrived, embeds, adds, layer_gain, final_gain, weights, final)
        if final:
            micro = t - fill
            pieces.append(got[1] if micro == sections - 1 else lax.ppermute(got[1], "section", [(sections - 1, micro)]))
        sent, arrived = got[0], coming
    total = sum(pieces[1:], pieces[0])
    return total[None]


def solution(mesh):
    in_specs = (
        P(None, "dp"), P(), P("section", "dp", None), P(), P("section", "dp", None),
        P("section", "dp", None), P("section", None), P(None, "dp"), P(), P(None, "dp"),
    )
    return jax.shard_map(shards, mesh=mesh, in_specs=in_specs, out_specs=P("section", "dp", None), check_vma=False)
```

```python
import functools

import jax
import jax.numpy as jnp
from jax import lax
from jax.experimental import pallas as pl
from jax.experimental.pallas import tpu as pltpu
from jax.sharding import PartitionSpec as P


PATCH = 8
HEAD_DIM = 64
GROUPS = 4
X_SIZE, Z_SIZE = 4, 8
SHARD = 16
VOCAB = 256


def norm_rows(hidden, gain):
    scale = lax.rsqrt(jnp.mean(hidden * hidden, axis=-1, keepdims=True) + 1e-06)
    return (hidden * scale * gain.astype(jnp.float32)).astype(jnp.bfloat16)


X_FROM = (0, -1, 1, 2)


def pack_body(place_ref, *refs):
    half, x, z = place_ref[0], place_ref[1], place_ref[2]
    near, ups, downs, up_far, down_far = refs[0], refs[1:4], refs[4:7], refs[7], refs[8]
    cross, cross_up, cross_down, cross_far_a, cross_far_b = refs[9:14]
    out_ref, sems = refs[14:]
    copies = []

    def move(source, target):
        copy = pltpu.make_async_copy(source, target, sems.at[len(copies)])
        copy.start()
        copies.append(copy)

    def at_z(step):
        return lax.rem(z + step + Z_SIZE, Z_SIZE)

    def at_x(step):
        return lax.rem(x + step + X_SIZE, X_SIZE)

    def move_columns(ref, step, first=0):
        for k in range(ref.shape[0]):
            move(ref.at[k], out_ref.at[half, at_x(X_FROM[first + k]), at_z(step)])

    move_columns(near, 0)
    for i in range(3):
        move_columns(ups[i], -1 - i)
        move_columns(downs[i], 1 + i)
    move_columns(up_far, 4)
    move_columns(down_far, 4, X_SIZE // 2)
    middle = Z_SIZE // 2
    move(cross, out_ref.at[1 - half, x])
    move(cross_up, out_ref.at[1 - half, at_x(-1)])
    move(cross_down, out_ref.at[1 - half, at_x(1)])
    move(cross_far_a, out_ref.at[1 - half, at_x(2), pl.ds(0, middle)])
    move(cross_far_b, out_ref.at[1 - half, at_x(2), pl.ds(middle, middle)])
    for copy in copies:
        copy.wait()


def pack_call(place, pieces):
    columns = pieces[0].shape[-1]
    return pl.pallas_call(
        pack_body,
        out_shape=jax.ShapeDtypeStruct((2, X_SIZE, Z_SIZE, SHARD, columns), jnp.bfloat16),
        in_specs=[pl.BlockSpec(memory_space=pltpu.SMEM)] + [pl.BlockSpec(memory_space=pl.ANY)] * len(pieces),
        out_specs=pl.BlockSpec(memory_space=pltpu.VMEM),
        scratch_shapes=[pltpu.SemaphoreType.DMA((X_SIZE * Z_SIZE + 5,))],
        compiler_params=pltpu.CompilerParams(vmem_limit_bytes=16 * 2 ** 20),
        name="pack",
    )(place, *pieces)


def neighbours(axis, step):
    pairs = []
    for h in range(2):
        for x in range(X_SIZE):
            for z in range(Z_SIZE):
                to_h, to_x, to_z = h, x, z
                if axis == "y":
                    to_h = (h + step) % 2
                elif axis == "x":
                    to_x = (x + step) % X_SIZE
                else:
                    to_z = (z + step) % Z_SIZE
                pairs.append(((h * X_SIZE + x) * Z_SIZE + z, (to_h * X_SIZE + to_x) * Z_SIZE + to_z))
    return pairs


def to_team(shard, teams):
    copies = jnp.broadcast_to(shard, (len(teams[0]), *shard.shape))
    return lax.all_to_all(copies, "dp", split_axis=0, concat_axis=0, axis_index_groups=teams, tiled=True)


def gather_plane(own):
    def shift(block, axis, step):
        return lax.ppermute(block, "dp", neighbours(axis, step))

    along_z = [[r * Z_SIZE + z for z in range(Z_SIZE)] for r in range(2 * X_SIZE)]
    other = shift(own, "y", 1)
    near = jnp.stack([own, shift(own, "x", 1), shift(own, "x", -1), shift(own, "x", 2)])
    ups, downs = [near], [near]
    for _ in range(3):
        ups.append(shift(ups[-1], "z", 1))
        downs.append(shift(downs[-1], "z", -1))
    up_far = shift(ups[-1][:X_SIZE // 2], "z", 1)
    down_far = shift(downs[-1][X_SIZE // 2:], "z", -1)
    cross = to_team(other, along_z)
    cross_up = shift(cross, "x", 1)
    cross_down = shift(cross, "x", -1)
    far_a = shift(cross_up[:Z_SIZE // 2], "x", 1)
    far_b = shift(cross_down[Z_SIZE // 2:], "x", -1)
    pieces = [near, *ups[1:], *downs[1:], up_far, down_far, cross, cross_up, cross_down, far_a, far_b]
    return pieces, near


def add_body(embed_ref, w_ref, out_ref):
    width = out_ref.shape[1]
    depth = embed_ref.shape[1]
    glob = w_ref[:, :, :, :, w_ref.shape[-1] - depth:].reshape(width, depth)
    out_ref[...] = lax.dot_general(embed_ref[...], glob, (((1,), (1,)), ((), ())),
                                   preferred_element_type=jnp.float32).astype(jnp.bfloat16)


def add_call(embeds, weights, width):
    vmem = pl.BlockSpec(memory_space=pltpu.VMEM)
    return pl.pallas_call(
        add_body,
        out_shape=jax.ShapeDtypeStruct((embeds.shape[0], width), jnp.bfloat16),
        in_specs=[vmem, vmem], out_specs=vmem,
        compiler_params=pltpu.CompilerParams(vmem_limit_bytes=24 * 2 ** 20),
        name="global_add",
    )(embeds, weights)


def attend(q, k, v, seen, head_of):
    rows, lanes = q.shape
    in_group = lanes // HEAD_DIM
    zero = jnp.zeros_like(q)
    spread = jnp.concatenate([jnp.where(head_of == j, q, zero) for j in range(in_group)], axis=0)
    scores = lax.dot_general(spread, k, (((1,), (1,)), ((), ())),
                             preferred_element_type=jnp.float32) * HEAD_DIM ** (-0.5)
    scores = jnp.where(seen, scores, -1e30)
    e = jnp.exp(scores - jnp.max(scores, axis=-1, keepdims=True))
    attn = (e / jnp.sum(e, axis=-1, keepdims=True)).astype(jnp.bfloat16)
    wide = jnp.dot(attn, v, preferred_element_type=jnp.float32)
    ctx = wide[:rows]
    for j in range(1, in_group):
        ctx = jnp.where(head_of == j, wide[j * rows:(j + 1) * rows], ctx)
    return ctx.astype(jnp.bfloat16)


def layer_body(final, t_ref, meta_ref, recv_ref, embed_ref, add_ref, gain_ref, final_gain_ref,
               w_ref, *rest):
    out_ref, ctx_buf = rest
    rows, width = out_ref.shape
    lanes = width // GROUPS
    micro_count = add_ref.shape[0]
    section = meta_ref[0]
    last_section = meta_ref[1]
    micro = t_ref[0] - 2 * section
    active = (micro >= 0) & (micro < micro_count)

    @pl.when(active)
    def _():
        x = jnp.where(section == 0, embed_ref[micro], recv_ref[...])
        hidden = x.astype(jnp.float32) + add_ref[micro].astype(jnp.float32)
        normed = norm_rows(hidden, gain_ref[...])
        row = lax.broadcasted_iota(jnp.int32, (rows, rows), 0)
        col = lax.broadcasted_iota(jnp.int32, (rows, rows), 1)
        seen = (row // PATCH == col // PATCH) & (col <= row)
        seen = jnp.concatenate([seen] * (lanes // HEAD_DIM), axis=0)
        head_of = lax.broadcasted_iota(jnp.int32, (rows, lanes), 1) // HEAD_DIM

        def project(at):
            w = w_ref[:, :, :, :, at:at + lanes].reshape(width, lanes)
            return jnp.dot(normed, w, preferred_element_type=jnp.float32).astype(jnp.bfloat16)

        projs = [[project(p * width + g * lanes) for p in range(3)] for g in range(GROUPS)]
        for g in range(GROUPS):
            ctx_buf[:, g * lanes:(g + 1) * lanes] = attend(*projs[g], seen, head_of)
        mixed = jnp.dot(ctx_buf[...], w_ref[:, :, :, :, 3 * width:4 * width].reshape(width, width),
                        preferred_element_type=jnp.float32)
        out_ref[...] = (hidden + mixed).astype(jnp.bfloat16)
        if final:
            @pl.when(section == last_section)
            def _():
                final_rows = norm_rows(out_ref[...].astype(jnp.float32), final_gain_ref[...])
                scores = jnp.dot(final_rows, w_ref[:, :, :, :, 4 * width:4 * width + VOCAB].reshape(width, VOCAB),
                                 preferred_element_type=jnp.float32)
                patch = meta_ref[2] + lax.broadcasted_iota(jnp.int32, scores.shape, 0) // PATCH
                live = patch < meta_ref[3 + micro]
                out_ref[:, :VOCAB] = jnp.where(live, scores, 0.0).astype(jnp.bfloat16)


def layer_call(t, meta, recv, embeds, adds, gain, final_gain, weights, final):
    rows, width = recv.shape
    vmem = pl.BlockSpec(memory_space=pltpu.VMEM)
    smem = pl.BlockSpec(memory_space=pltpu.SMEM)
    x_shape = jax.ShapeDtypeStruct((rows, width), jnp.bfloat16)
    scratch = [pltpu.VMEM((rows, width), jnp.bfloat16)]
    return pl.pallas_call(
        functools.partial(layer_body, final),
        out_shape=x_shape,
        in_specs=[smem, smem] + [vmem] * 6,
        out_specs=vmem,
        scratch_shapes=scratch,
        compiler_params=pltpu.CompilerParams(vmem_limit_bytes=8 * 2 ** 20),
        cost_estimate=pl.CostEstimate(flops=8 * rows * width * width, bytes_accessed=8 * width * width,
                                      transcendentals=rows * rows * 16),
        name="layer_final" if final else "layer",
    )(t, meta, recv, embeds, adds, gain, final_gain, weights)


def pick_body(meta_ref, *refs):
    for micro, ref in enumerate(refs[:-1]):
        @pl.when(meta_ref[0] == micro)
        def _():
            refs[-1][...] = ref[:, :VOCAB]


def pick_call(meta, blocks):
    vmem = pl.BlockSpec(memory_space=pltpu.VMEM)
    return pl.pallas_call(
        pick_body,
        out_shape=jax.ShapeDtypeStruct((blocks[0].shape[0], VOCAB), jnp.bfloat16),
        in_specs=[pl.BlockSpec(memory_space=pltpu.SMEM)] + [vmem] * len(blocks),
        out_specs=vmem,
        compiler_params=pltpu.CompilerParams(vmem_limit_bytes=8 * 2 ** 20),
        name="pick",
    )(meta, *blocks)


def previous_bytes(byte_ids):
    blocks = byte_ids.reshape(-1, PATCH)
    shifted = jnp.concatenate([jnp.zeros((blocks.shape[0], 1), jnp.int32), blocks[:, :-1]], axis=1)
    return shifted.reshape(-1)


def shards(tokens, doc_patches, global_embed, byte_table, w_qkv, w_out, layer_gain, w_global,
           final_gain, w_head):
    sections = lax.axis_size("section")
    section = lax.axis_index("section")
    column = lax.axis_index("dp")
    micro_count, row_count = tokens.shape
    width = byte_table.shape[1]

    own = jnp.concatenate([w_qkv[0], w_out[0], w_head.T, w_global.T], axis=1)
    pieces, near = gather_plane(own)

    copies = jnp.broadcast_to(global_embed, (sections, *global_embed.shape[1:]))
    copies, _ = lax.optimization_barrier((copies, near))
    globals_ = lax.all_to_all(copies, "section", split_axis=0, concat_axis=0, tiled=True)
    globals_ = globals_.reshape(micro_count * row_count, -1)

    pieces[0], globals_ = lax.optimization_barrier((pieces[0], globals_))
    place = jnp.stack([column // (X_SIZE * Z_SIZE), column // Z_SIZE % X_SIZE, column % Z_SIZE]).astype(jnp.int32)
    weights = pack_call(place, pieces)

    byte_ids = previous_bytes(tokens.reshape(-1))
    one_hot = (byte_ids[:, None] == jnp.arange(byte_table.shape[0], dtype=jnp.int32)[None, :]).astype(jnp.bfloat16)
    embeds = jnp.dot(one_hot, byte_table, preferred_element_type=jnp.float32).astype(jnp.bfloat16)
    embeds = embeds.reshape(micro_count, row_count, width)
    adds = add_call(globals_, weights, width).reshape(micro_count, row_count, width)

    meta = jnp.concatenate([
        jnp.stack([section, jnp.int32(sections - 1), column * (row_count // PATCH)]).astype(jnp.int32),
        doc_patches])
    final_gain = final_gain.reshape(1, width)

    fill = 2 * (sections - 1)
    steps = fill + micro_count

    def send(t, block):
        onward = [(s, s + 1) for s in range(sections - 1) if 0 <= t - 2 * s < micro_count]
        if t >= fill:
            onward.append((sections - 1, t - fill))
        return lax.ppermute(block, "section", onward)

    arrived = jnp.zeros((row_count, width), jnp.bfloat16)
    sent = None
    finished = []
    for t in range(steps):
        coming = send(t - 1, sent) if t > 0 else arrived
        if t > fill:
            finished.append(coming)
        got = layer_call(jnp.full((1,), t, jnp.int32), meta, arrived, embeds, adds, layer_gain, final_gain, weights, t >= fill)
        sent, arrived = got, coming
    total = pick_call(meta, [*finished, sent])
    return total[None]


def solution(mesh):
    in_specs = (
        P(None, "dp"), P(), P("section", "dp", None), P(), P("section", "dp", None),
        P("section", "dp", None), P("section", None), P(None, "dp"), P(), P(None, "dp"),
    )
    return jax.shard_map(shards, mesh=mesh, in_specs=in_specs, out_specs=P("section", "dp", None), check_vma=False)
```
